32 devices in a mesh: grp: 4 (over y, x), chan: 8 (over z, core).
Axes of the slice: x: 2, y: 2, z: 4, core: 2. Of those that a mesh axis runs over, the one named last changes fastest.
Arguments:
- visibility: float32 [1024, 32768], P('chan', 'grp'), may hold values from -6 to 6
- interference_mask: int32 [1024, 16384], P(None, ('grp', 'chan')), may hold values from 0 to 1
- valid_time_count: int32 [512], P(('grp', 'chan')), may hold values from 8 to 32
- fit_modes: float32 [1024, 32], P('grp'), may hold values from -1 to 1
Outputs:
- residual_vis: float32 [1024, 32768], P('chan', 'grp')
The draws below stay inside these ranges and needn't reach their ends.
All inputs are finite; a program needn't handle non-finite values.
Results may differ from the reference program's by a relative error of at most 0.0003.
Values sent between devices are 32-bit elements; how exact they have to be, the bound alone decides.
A program may use at most 128 MiB of HBM per device.

```python
import jax
import jax.numpy as jnp
from jax import lax

FREQ = 1024
MODES = 32
NT = 32
BASE_DEV = 16
BASE = 512
N_GRP = 4
N_CHAN = 8


def draw_interference_mask(key, part):
    start_key = jax.random.fold_in(key, 11)
    length_key = jax.random.fold_in(key, 12)
    speck_key = jax.random.fold_in(key, 13)
    columns = BASE * NT
    band_start = jax.random.randint(start_key, (1, columns), 0, FREQ, dtype=jnp.int32)
    band_length = jax.random.randint(length_key, (1, columns), 0, FREQ * 7 // 8 + 1, dtype=jnp.int32)
    freq_index = lax.broadcasted_iota(jnp.int32, (FREQ, columns), 0)
    inside_band = (freq_index >= band_start) & (freq_index < band_start + band_length)
    scattered = jax.random.randint(speck_key, (FREQ, columns), 0, 16, dtype=jnp.int32) == 0
    return (inside_band | scattered).astype(jnp.int32)


def draw_fit_modes(key, part):
    center_key = jax.random.fold_in(key, 21)
    rough_key = jax.random.fold_in(key, 22)
    centers = jax.random.uniform(center_key, (1, MODES), jnp.float32, 0.0, 1.0) * FREQ
    freq_index = lax.broadcasted_iota(jnp.float32, (FREQ, MODES), 0)
    spread = FREQ / 6.0
    offset = (freq_index - centers) / spread
    envelope = 0.25 + 1.75 * jnp.exp(-0.5 * offset * offset)
    rough = jnp.clip(jax.random.normal(rough_key, (FREQ, MODES), jnp.float32), -4.0, 4.0)
    column_scale = jnp.sqrt(jnp.sum(envelope * envelope, axis=0, keepdims=True))
    return jnp.clip(rough * envelope / column_scale, -1.0, 1.0)


def plant(values, own_key, least, top_value):
    extent = values.shape
    index_at = [jax.random.randint(jax.random.fold_in(own_key, axis), (), 0, extent[axis]) for axis in range(len(extent))]
    values = values.at[tuple(index_at)].set(least)
    longest = extent.index(max(extent))
    index_at[longest] = (index_at[longest] + 1) % extent[longest]
    return values.at[tuple(index_at)].set(top_value)


def levels(own_key, shape, pieces, smallest, largest):
    level = 1.0
    for dim, parts in pieces:
        heights = jax.random.uniform(jax.random.fold_in(jax.random.fold_in(own_key, 6), dim), (parts,), jnp.float32, smallest / len(pieces), largest / len(pieces))
        level = level * jnp.repeat(jnp.exp(heights), shape[dim] // parts).reshape((-1,) + (1,) * (len(shape) - 1 - dim))
    return level


def noise(stream_key, dims, width, limit, cuts=(), held_as=jnp.bfloat16):
    values = jax.random.normal(stream_key, dims, jnp.float32) * width
    if len(cuts) > 0:
        values = levels(stream_key, dims, cuts, -0.22, 0.18) * values
    return jnp.clip(values, min=-limit, max=limit).astype(held_as)


def setup_inputs(seed: int = 0) -> dict:
    seeds = jax.random.split(jax.random.key(seed), 5)
    return {
        "visibility": noise(seeds[0], (FREQ, BASE * 2 * NT), 1.0, 6.0, ((0, 8), (1, 4)), jnp.float32),
        "interference_mask": draw_interference_mask(jax.random.fold_in(seeds[4], 71), 0),
        "valid_time_count": plant(jax.random.randint(seeds[2], (BASE,), NT // 4, NT + 1), jax.random.fold_in(seeds[2], 1), NT // 4, NT).astype(jnp.int32),
        "fit_modes": draw_fit_modes(jax.random.fold_in(seeds[4], 71), 0),
    }


damping = 0.1

def fit_weight(interference_mask, valid_time_count):
    antenna_pairs_list = valid_time_count.shape[0]
    sample_values = interference_mask.shape[1] // antenna_pairs_list
    projection_sums = lax.broadcasted_iota(jnp.int32, (antenna_pairs_list, sample_values), 1)
    within_range = (projection_sums < valid_time_count[:, None]).astype(jnp.float32).reshape(1, antenna_pairs_list * sample_values)
    return (1.0 - interference_mask.astype(jnp.float32)) * within_range

def solve_normal(normal_matrix, target_signal):
    span_length = normal_matrix.shape[0]
    trailing = normal_matrix
    columns = []
    for position in range(span_length):
        column = trailing[:, 0] / jnp.sqrt(trailing[0, 0])
        columns.append(column)
        trailing = trailing[1:, 1:] - column[1:, None, :] * column[None, 1:, :]
    remains = target_signal
    forward = []
    for position in range(span_length):
        column = columns[position]
        current = remains[0] / column[0][None, :]
        forward.append(current)
        remains = remains[1:] - column[1:, None, :] * current[None]
    solution_values = [None] * span_length
    for position in reversed(range(span_length)):
        column = columns[position]
        current = forward[position]
        if position + 1 < span_length:
            later_rows = jnp.stack(solution_values[position + 1:], 0)
            current = current - lax.optimization_barrier(jnp.sum(column[1:, None, :] * later_rows, axis=0))
        solution_values[position] = current / column[0][None, :]
    return jnp.stack(solution_values, 0)

def solve_amplitudes(spectral_templates, assigned_rows, sample_weight, antenna_pairs_list):
    channel_count, span_length = spectral_templates.shape
    sample_values = sample_weight.shape[1] // antenna_pairs_list
    pairs = (spectral_templates[:, :, None] * spectral_templates[:, None, :]).reshape(channel_count, span_length * span_length)
    normal_matrix = lax.dot_general(pairs, sample_weight, (((0,), (0,)), ((), ())), precision=lax.Precision.HIGHEST, preferred_element_type=jnp.float32)
    normal_matrix = normal_matrix.reshape(span_length, span_length, antenna_pairs_list * sample_values)
    normal_matrix = normal_matrix + damping * jnp.eye(span_length, dtype=normal_matrix.dtype)[:, :, None]
    weighted_values = assigned_rows.reshape(channel_count, antenna_pairs_list, 2, sample_values) * sample_weight.reshape(channel_count, antenna_pairs_list, 1, sample_values)
    weighted_values = weighted_values.reshape(channel_count, antenna_pairs_list * 2 * sample_values)
    template_projection = lax.dot_general(spectral_templates, weighted_values, (((0,), (0,)), ((), ())), precision=lax.Precision.HIGHEST, preferred_element_type=jnp.float32)
    target_signal = template_projection.reshape(span_length, antenna_pairs_list, 2, sample_values).transpose(0, 2, 1, 3).reshape(span_length, 2, antenna_pairs_list * sample_values)
    solution_values = solve_normal(normal_matrix, target_signal)
    return solution_values.reshape(span_length, 2, antenna_pairs_list, sample_values).transpose(0, 2, 1, 3).reshape(span_length, antenna_pairs_list * 2 * sample_values)

def reference(visibility, interference_mask, valid_time_count, fit_modes):
    blocks = N_GRP * N_CHAN
    stacked = visibility.reshape(FREQ, blocks, BASE_DEV * 2 * NT).transpose(1, 0, 2)
    flagged = interference_mask.reshape(FREQ, blocks, BASE_DEV * NT).transpose(1, 0, 2)
    counted = valid_time_count.reshape(blocks, BASE_DEV)

    def one_block(items):
        assigned_rows, block_flags, block_counts = items
        sample_weight = fit_weight(block_flags, block_counts)
        mode_amplitudes = solve_amplitudes(fit_modes, assigned_rows, sample_weight, BASE_DEV)
        model = jnp.dot(fit_modes, mode_amplitudes, precision=lax.Precision.HIGHEST, preferred_element_type=jnp.float32)
        return assigned_rows - model
    result = lax.map(one_block, (stacked, flagged, counted))
    return result.transpose(1, 0, 2).reshape(FREQ, BASE * 2 * NT)
```

```python
import functools

import jax
import jax.numpy as jnp
from jax import lax
from jax.experimental import pallas as pl
from jax.experimental.pallas import tpu as pltpu
from jax.sharding import PartitionSpec as P

damping = 0.1
LANES = 128
VMEM = pl.BlockSpec(memory_space=pltpu.VMEM)
MESH = pl.DeviceIdType.MESH


def factor_kernel(mt_ref, mask_ref, valid_ref, spread_ref, l_ref, inv_ref, w_ref, hi_ref, mid_ref, lo_ref):
    modes, freqs = mt_ref.shape
    columns = mask_ref.shape[1]
    for j in range(columns // LANES):
        part = slice(j * LANES, (j + 1) * LANES)
        w = (1.0 - mask_ref[:, part].astype(jnp.float32)) * valid_ref[:, part]
        w_ref[:, 2 * j * LANES : 2 * (j + 1) * LANES] = jnp.dot(
            w.astype(jnp.bfloat16), spread_ref[...], preferred_element_type=jnp.float32
        ).astype(jnp.bfloat16)

    def split(i, carry):
        pair = mt_ref[...] * mt_ref[pl.ds(i, 1), :]
        rows = pl.ds(pl.multiple_of(i * modes, modes), modes)
        hi = pair.astype(jnp.bfloat16)
        rest = pair - hi.astype(jnp.float32)
        mid = rest.astype(jnp.bfloat16)
        hi_ref[rows, :] = hi
        mid_ref[rows, :] = mid
        lo_ref[rows, :] = (rest - mid.astype(jnp.float32)).astype(jnp.bfloat16)
        return carry

    lax.fori_loop(0, modes, split, 0)
    tile, group = 2 * LANES, 8

    def gram(step, carry):
        cols = pl.ds(pl.multiple_of(step // (modes // group) * tile, tile), tile)
        first = step % (modes // group)
        rows = pl.ds(pl.multiple_of(first * group * modes, group * modes), group * modes)
        w = w_ref[:, cols]
        total = jnp.dot(lo_ref[rows, :], w, preferred_element_type=jnp.float32)
        total += jnp.dot(mid_ref[rows, :], w, preferred_element_type=jnp.float32)
        total += jnp.dot(hi_ref[rows, :], w, preferred_element_type=jnp.float32)
        l_ref[pl.ds(first * group, group), :, cols] = total.reshape(group, modes, tile)
        return carry

    lax.fori_loop(0, 2 * columns // tile * (modes // group), gram, 0)
    width = 4 * LANES

    def cholesky(step, carry):
        cols = pl.ds(pl.multiple_of(step * width, width), width)
        for k in range(modes):
            low = k // 8 * 8
            row = lax.broadcasted_iota(jnp.int32, (modes - low, width), 0) + low
            acc = l_ref[k, low:, cols] + jnp.where(row == k, damping, 0.0)
            for m in range(k):
                acc = acc - l_ref[m, low:, cols] * l_ref[m, k : k + 1, cols]
            inv = 1.0 / jnp.sqrt(acc[k - low : k - low + 1])
            inv_ref[k : k + 1, cols] = inv
            l_ref[k, low:, cols] = acc * inv
        return carry

    lax.fori_loop(0, 2 * columns // width, cholesky, 0)


def fit_kernel(chips, vis_ref, mask_ref, mt_ref, spread_ref, valid_ref, l_ref, inv_ref, out_ref,
               give, keep, take, sums, come, sems):
    me = lax.axis_index("chan")
    chip, core = me // 2, me % 2
    modes, width = inv_ref.shape
    columns = mask_ref.shape[2]
    barrier = pltpu.get_barrier_semaphore()
    pl.semaphore_signal(barrier, inc=1, device_id={"chan": chip * 2 + 1 - core}, device_id_type=MESH)
    for d in range(1, chips):
        peer = lax.rem(chip + d, chips)
        pl.semaphore_signal(barrier, inc=1, device_id={"chan": peer * 2 + core}, device_id_type=MESH)
    pl.semaphore_wait(barrier, chips)

    def copy(stage, src, dst, slot, peer, at):
        return pltpu.make_async_remote_copy(
            src_ref=src, dst_ref=dst, send_sem=sems.at[2 * stage, slot], recv_sem=sems.at[2 * stage + 1, at],
            device_id={"chan": peer}, device_id_type=MESH)

    mate = chip * 2 + 1 - core

    def project(owner, dst, slot):
        for j in range(columns // LANES):
            w = 1.0 - mask_ref[owner, :, j * LANES : (j + 1) * LANES].astype(jnp.float32)
            w = jnp.dot(w.astype(jnp.bfloat16), spread_ref[...], preferred_element_type=jnp.float32)
            at = pl.multiple_of(owner * width + 2 * j * LANES, 2 * LANES)
            v = vis_ref[:, pl.ds(at, 2 * LANES)] * w
            dst[slot, :, 2 * j * LANES : 2 * (j + 1) * LANES] = jnp.dot(
                mt_ref[...], v, precision=lax.Precision.HIGHEST, preferred_element_type=jnp.float32)

    def theirs(d, carry):
        slot = lax.rem(chip + d, chips)
        project(slot * 2 + 1 - core, give, slot)
        copy(0, give.at[slot], take.at[slot], slot, mate, slot).start()
        return carry

    lax.fori_loop(1, chips + 1, theirs, 0)

    def mine(d, carry):
        slot = lax.rem(chip + d, chips)
        project(slot * 2 + core, keep, slot)
        return carry

    lax.fori_loop(1, chips + 1, mine, 0)
    for d in range(1, chips + 1):
        slot = lax.rem(chip + d, chips)
        copy(0, give.at[slot], take.at[slot], slot, mate, slot).wait()
        if d < chips:
            sums[slot] = keep[slot] + take[slot]
            copy(1, sums.at[slot], come.at[chip], slot, slot * 2 + core, chip).start()
    total = keep[chip] + take[chip]
    for d in range(1, chips):
        slot = lax.rem(chip + d, chips)
        copy(1, sums.at[slot], come.at[slot], slot, slot * 2 + core, slot).wait()
        total = total + come[slot]
    take[chip] = total * valid_ref[...]

    part = 2 * LANES

    def solve(step, carry):
        cols = pl.ds(pl.multiple_of(step * part, part), part)
        row = lax.broadcasted_iota(jnp.int32, (modes, part), 0)
        left = take[chip, :, cols]
        groups = [left[g * 8 : (g + 1) * 8] for g in range(modes // 8)]
        ys = []
        for k in range(modes):
            low = k // 8
            y = groups[low][k % 8 : k % 8 + 1] * inv_ref[k : k + 1, cols]
            ys.append(y)
            for g in range(low, modes // 8):
                groups[g] = groups[g] - l_ref[k, g * 8 : (g + 1) * 8, cols] * y
        row = lax.broadcasted_iota(jnp.int32, (8, part), 0)
        xs = [jnp.zeros((8, part), jnp.float32) for _ in range(modes // 8)]
        for k in reversed(range(modes)):
            low = k // 8
            acc = l_ref[k, low * 8 : (low + 1) * 8, cols] * xs[low]
            for g in range(low + 1, modes // 8):
                acc = acc + l_ref[k, g * 8 : (g + 1) * 8, cols] * xs[g]
            x = (ys[k] - jnp.sum(acc, axis=0, keepdims=True)) * inv_ref[k : k + 1, cols]
            xs[low] = jnp.where(row == k % 8, x, xs[low])
        for g in range(modes // 8):
            out_ref[me, g * 8 : (g + 1) * 8, cols] = xs[g]
        return carry

    lax.fori_loop(0, width // part, solve, 0)

    def spread(slot):
        block = out_ref.at[slot * 2 + core]
        return copy(3, block, block, slot, mate, slot)

    for d in range(1, chips):
        slot = lax.rem(chip + d, chips)
        copy(2, out_ref.at[me], out_ref.at[me], slot, slot * 2 + core, chip).start()
    spread(chip).start()
    for d in range(1, chips):
        slot = lax.rem(chip + d, chips)
        block = out_ref.at[slot * 2 + core]
        copy(2, block, block, slot, slot * 2 + core, slot).wait_recv()
        spread(slot).start()
    for d in range(1, chips):
        slot = lax.rem(chip + d, chips)
        copy(2, out_ref.at[me], out_ref.at[me], slot, slot * 2 + core, chip).wait_send()
    for slot in range(chips):
        block = out_ref.at[slot * 2 + 1 - core]
        spread(slot).wait_send()
        copy(3, block, block, slot, mate, slot).wait_recv()


def residual_kernel(vis_ref, modes_ref, coef_ref, out_ref):
    width = coef_ref.shape[2]
    for j in range(coef_ref.shape[0]):
        cols = slice(j * width, (j + 1) * width)
        out_ref[:, cols] = vis_ref[:, cols] - jnp.dot(
            modes_ref[...], coef_ref[j], precision=lax.Precision.HIGHEST, preferred_element_type=jnp.float32)


def per_device(chan, visibility, interference_mask, valid_time_count, fit_modes):
    rows, all_columns = visibility.shape
    freqs, columns = interference_mask.shape
    modes = fit_modes.shape[1]
    base = valid_time_count.shape[0]
    times = columns // base
    width = 2 * columns
    chips = chan // 2
    flags = lax.all_to_all(interference_mask.reshape(chan, rows, columns), "chan", 0, 0)
    table = lax.all_gather(fit_modes, "grp", axis=0, tiled=True)
    local = lax.dynamic_slice_in_dim(table, lax.axis_index("chan") * rows, rows, 0)
    within = (lax.broadcasted_iota(jnp.int32, (base, times), 1) < valid_time_count[:, None]).astype(jnp.float32)
    valid = within.reshape(1, columns)
    valid_wide = jnp.broadcast_to(within[:, None, :], (base, 2, times)).reshape(1, width)
    source = lax.broadcasted_iota(jnp.int32, (LANES, 2 * LANES), 0)
    column = lax.broadcasted_iota(jnp.int32, (LANES, 2 * LANES), 1)
    spread = (source == column // (2 * times) * times + column % times).astype(jnp.bfloat16)
    f32 = jnp.float32
    factor, inverse = pl.pallas_call(
        factor_kernel,
        out_shape=(jax.ShapeDtypeStruct((modes, modes, width), f32), jax.ShapeDtypeStruct((modes, width), f32)),
        in_specs=[VMEM] * 4,
        out_specs=(VMEM, VMEM),
        scratch_shapes=[pltpu.VMEM((freqs, width), jnp.bfloat16)]
        + [pltpu.VMEM((modes * modes, freqs), jnp.bfloat16)] * 3,
        compiler_params=pltpu.CompilerParams(vmem_limit_bytes=40 << 20),
        cost_estimate=pl.CostEstimate(flops=20 * 10**9, bytes_accessed=8 << 20, transcendentals=0),
        name="factor",
    )(table.T, interference_mask, valid, spread)
    block = pltpu.VMEM((chips, modes, width), f32)
    coefficients = pl.pallas_call(
        functools.partial(fit_kernel, chips),
        out_shape=jax.ShapeDtypeStruct((chan, modes, width), f32),
        in_specs=[VMEM] * 7,
        out_specs=VMEM,
        scratch_shapes=[block] * 5 + [pltpu.SemaphoreType.DMA((8, chips))],
        compiler_params=pltpu.CompilerParams(
            collective_id=0, has_side_effects=True, vmem_limit_bytes=56 << 20),
        cost_estimate=pl.CostEstimate(flops=10**10, bytes_accessed=12 << 20, transcendentals=0),
        name="fit",
    )(visibility, flags, local.T, spread, valid_wide, factor, inverse)
    step = 2
    return pl.pallas_call(
        residual_kernel,
        grid=(chan // step,),
        out_shape=jax.ShapeDtypeStruct((rows, all_columns), f32),
        in_specs=[
            pl.BlockSpec((rows, step * width), lambda i: (0, i)),
            pl.BlockSpec((rows, modes), lambda i: (0, 0)),
            pl.BlockSpec((step, modes, width), lambda i: (i, 0, 0)),
        ],
        out_specs=pl.BlockSpec((rows, step * width), lambda i: (0, i)),
        name="residual",
    )(visibility, local, coefficients)


def solution(mesh):
    placed = (P("chan", "grp"), P(None, ("grp", "chan")), P(("grp", "chan")), P("grp", None))
    return jax.shard_map(
        functools.partial(per_device, mesh.shape["chan"]), mesh=mesh, in_specs=placed, out_specs=P("chan", "grp"),
        check_vma=False)
```

```python
import functools

import jax
import jax.numpy as jnp
from jax import lax
from jax.experimental import pallas as pl
from jax.experimental.pallas import tpu as pltpu
from jax.sharding import PartitionSpec as P

damping = 0.1
LANES = 128
VMEM = pl.BlockSpec(memory_space=pltpu.VMEM)
MESH = pl.DeviceIdType.MESH


def factor_kernel(mt_ref, mask_ref, valid_ref, spread_ref, l_ref, inv_ref, w_ref, hi_ref, mid_ref, lo_ref):
    modes, freqs = mt_ref.shape
    columns = mask_ref.shape[1]
    for j in range(columns // LANES):
        part = slice(j * LANES, (j + 1) * LANES)
        w = (1.0 - mask_ref[:, part].astype(jnp.float32)) * valid_ref[:, part]
        w_ref[:, 2 * j * LANES : 2 * (j + 1) * LANES] = jnp.dot(
            w.astype(jnp.bfloat16), spread_ref[...], preferred_element_type=jnp.float32
        ).astype(jnp.bfloat16)

    def split(i, carry):
        pair = mt_ref[...] * mt_ref[pl.ds(i, 1), :]
        rows = pl.ds(pl.multiple_of(i * modes, modes), modes)
        hi = pair.astype(jnp.bfloat16)
        rest = pair - hi.astype(jnp.float32)
        mid = rest.astype(jnp.bfloat16)
        hi_ref[rows, :] = hi
        mid_ref[rows, :] = mid
        lo_ref[rows, :] = (rest - mid.astype(jnp.float32)).astype(jnp.bfloat16)
        return carry

    lax.fori_loop(0, modes, split, 0)
    tile, group = 2 * LANES, 8

    def gram(step, carry):
        cols = pl.ds(pl.multiple_of(step // (modes // group) * tile, tile), tile)
        first = step % (modes // group)
        rows = pl.ds(pl.multiple_of(first * group * modes, group * modes), group * modes)
        w = w_ref[:, cols]
        total = jnp.dot(lo_ref[rows, :], w, preferred_element_type=jnp.float32)
        total += jnp.dot(mid_ref[rows, :], w, preferred_element_type=jnp.float32)
        total += jnp.dot(hi_ref[rows, :], w, preferred_element_type=jnp.float32)
        l_ref[pl.ds(first * group, group), :, cols] = total.reshape(group, modes, tile)
        return carry

    lax.fori_loop(0, 2 * columns // tile * (modes // group), gram, 0)
    width = 4 * LANES

    def cholesky(step, carry):
        cols = pl.ds(pl.multiple_of(step * width, width), width)
        for k in range(modes):
            low = k // 8 * 8
            row = lax.broadcasted_iota(jnp.int32, (modes - low, width), 0) + low
            acc = l_ref[k, low:, cols] + jnp.where(row == k, damping, 0.0)
            for m in range(k):
                acc = acc - l_ref[m, low:, cols] * l_ref[m, k : k + 1, cols]
            inv = 1.0 / jnp.sqrt(acc[k - low : k - low + 1])
            inv_ref[k : k + 1, cols] = inv
            l_ref[k, low:, cols] = acc * inv
        return carry

    lax.fori_loop(0, 2 * columns // width, cholesky, 0)


def fit_kernel(chips, groups, vis_hbm, mask_hbm, share_ref, spread_ref, valid_ref, wide_ref, out_ref, loc_ref,
               vis_ref, own_ref, mask_ref, table, mt_all, w_ref, hi_ref, mid_ref, lo_ref, l_ref, inv_ref,
               give, keep, take, sums, come, sems, mask_sems, table_sems, local_sems):
    me, grp = lax.axis_index("chan"), lax.axis_index("grp")
    chip, core = me // 2, me % 2
    turn = 1 - 2 * (2 * chip // chips)
    modes, width = inv_ref.shape
    rows = vis_ref.shape[0]
    columns = mask_ref.shape[2]
    share = share_ref.shape[1]
    mate = chip * 2 + 1 - core

    def other(d):
        return lax.rem(chip + turn * d + chips, chips)

    load_own = pltpu.make_async_copy(mask_hbm, own_ref, local_sems.at[0])
    load_own.start()
    barrier = pltpu.get_barrier_semaphore()
    for d in range(1, 2 * chips):
        pl.semaphore_signal(barrier, inc=1, device_id={"chan": lax.rem(me + d, 2 * chips)}, device_id_type=MESH)
    for d in range(1, groups):
        pl.semaphore_signal(barrier, inc=1, device_id={"grp": lax.rem(grp + d, groups)}, device_id_type=MESH)
    pl.semaphore_wait(barrier, 2 * chips + groups - 2)

    def flags(peer, slot, at):
        return pltpu.make_async_remote_copy(
            src_ref=mask_hbm.at[pl.ds(pl.multiple_of(peer * rows, rows), rows)], dst_ref=mask_ref.at[slot],
            send_sem=mask_sems.at[0, peer], recv_sem=mask_sems.at[1, at],
            device_id={"chan": peer}, device_id_type=MESH)

    def modes_copy(peer, slot):
        return pltpu.make_async_remote_copy(
            src_ref=share_ref, dst_ref=table.at[slot], send_sem=table_sems.at[0, peer],
            recv_sem=table_sems.at[1, slot], device_id={"grp": peer}, device_id_type=MESH)

    for d in range(1, groups):
        modes_copy(lax.rem(grp + d, groups), grp).start()
    flags(mate, me, me).start()
    for d in range(1, chips):
        flags(other(d) * 2 + core, me, me).start()
        flags(other(d) * 2 + 1 - core, me, me).start()
    load_vis = pltpu.make_async_copy(vis_hbm, vis_ref, local_sems.at[1])
    load_vis.start()
    load_mine = pltpu.make_async_copy(
        mask_hbm.at[pl.ds(pl.multiple_of(me * rows, rows), rows)], mask_ref.at[me], local_sems.at[2])
    load_mine.start()

    table[grp] = share_ref[...]
    for d in range(1, groups):
        peer = lax.rem(grp + d, groups)
        modes_copy(peer, peer).wait_recv()
    for q in range(groups):
        mt_all[:, q * share : (q + 1) * share] = table[q]
    pick = lax.broadcasted_iota(jnp.int32, (groups * share, rows), 0)
    pick = pick == lax.broadcasted_iota(jnp.int32, (groups * share, rows), 1) + me * rows
    loc_ref[...] = jnp.dot(mt_all[...], pick.astype(jnp.float32),
                           precision=lax.Precision.HIGHEST, preferred_element_type=jnp.float32)
    load_own.wait()
    factor_kernel(mt_all, own_ref, valid_ref, spread_ref, l_ref, inv_ref, w_ref, hi_ref, mid_ref, lo_ref)
    load_vis.wait()
    load_mine.wait()

    def copy(stage, src, dst, slot, peer, at):
        return pltpu.make_async_remote_copy(
            src_ref=src, dst_ref=dst, send_sem=sems.at[2 * stage, slot], recv_sem=sems.at[2 * stage + 1, at],
            device_id={"chan": peer}, device_id_type=MESH)

    def project(owner, dst, slot):
        for j in range(columns // LANES):
            w = 1.0 - mask_ref[owner, :, j * LANES : (j + 1) * LANES].astype(jnp.float32)
            w = jnp.dot(w.astype(jnp.bfloat16), spread_ref[...], preferred_element_type=jnp.float32)
            at = pl.multiple_of(owner * width + 2 * j * LANES, 2 * LANES)
            v = vis_ref[:, pl.ds(at, 2 * LANES)] * w
            dst[slot, :, 2 * j * LANES : 2 * (j + 1) * LANES] = jnp.dot(
                loc_ref[...], v, precision=lax.Precision.HIGHEST, preferred_element_type=jnp.float32)

    flags(mate, mate, mate).wait_recv()
    project(mate, give, chip)
    pair = copy(0, give.at[chip], take.at[chip], chip, mate, chip)
    pair.start()
    project(me, keep, chip)
    pair.wait()

    def collect(d, carry):
        slot = other(d)
        first, second = slot * 2 + 1 - core, slot * 2 + core
        flags(first, first, first).wait_recv()
        project(first, give, slot)
        pair = copy(0, give.at[slot], take.at[slot], slot, mate, slot)
        pair.start()
        flags(second, second, second).wait_recv()
        project(second, keep, slot)
        pair.wait()
        sums[slot] = keep[slot] + take[slot]
        copy(1, sums.at[slot], come.at[chip], slot, slot * 2 + core, chip).start()
        return carry

    lax.fori_loop(1, chips, collect, 0)
    total = keep[chip] + take[chip]
    for d in range(1, chips):
        slot = other(d)
        copy(1, sums.at[slot], come.at[slot], slot, slot * 2 + core, slot).wait()
        total = total + come[slot]
    take[chip] = total * wide_ref[...]

    part = 2 * LANES

    def solve(step, carry):
        cols = pl.ds(pl.multiple_of(step * part, part), part)
        row = lax.broadcasted_iota(jnp.int32, (modes, part), 0)
        left = take[chip, :, cols]
        groups = [left[g * 8 : (g + 1) * 8] for g in range(modes // 8)]
        ys = []
        for k in range(modes):
            low = k // 8
            y = groups[low][k % 8 : k % 8 + 1] * inv_ref[k : k + 1, cols]
            ys.append(y)
            for g in range(low, modes // 8):
                groups[g] = groups[g] - l_ref[k, g * 8 : (g + 1) * 8, cols] * y
        row = lax.broadcasted_iota(jnp.int32, (8, part), 0)
        xs = [jnp.zeros((8, part), jnp.float32) for _ in range(modes // 8)]
        for k in reversed(range(modes)):
            low = k // 8
            acc = l_ref[k, low * 8 : (low + 1) * 8, cols] * xs[low]
            for g in range(low + 1, modes // 8):
                acc = acc + l_ref[k, g * 8 : (g + 1) * 8, cols] * xs[g]
            x = (ys[k] - jnp.sum(acc, axis=0, keepdims=True)) * inv_ref[k : k + 1, cols]
            xs[low] = jnp.where(row == k % 8, x, xs[low])
        for g in range(modes // 8):
            out_ref[me, g * 8 : (g + 1) * 8, cols] = xs[g]
        return carry

    lax.fori_loop(0, width // part, solve, 0)

    def spread(slot):
        block = out_ref.at[slot * 2 + core]
        return copy(3, block, block, slot, mate, slot)

    for d in range(1, chips):
        slot = lax.rem(chip + d, chips)
        copy(2, out_ref.at[me], out_ref.at[me], slot, slot * 2 + core, chip).start()
    spread(chip).start()
    for d in range(1, chips):
        slot = lax.rem(chip + d, chips)
        block = out_ref.at[slot * 2 + core]
        copy(2, block, block, slot, slot * 2 + core, slot).wait_recv()
        spread(slot).start()
    for d in range(1, chips):
        slot = lax.rem(chip + d, chips)
        copy(2, out_ref.at[me], out_ref.at[me], slot, slot * 2 + core, chip).wait_send()
    for slot in range(chips):
        block = out_ref.at[slot * 2 + 1 - core]
        spread(slot).wait_send()
        copy(3, block, block, slot, mate, slot).wait_recv()
    flags(mate, me, me).wait_send()
    for d in range(1, chips):
        flags(other(d) * 2 + core, me, me).wait_send()
        flags(other(d) * 2 + 1 - core, me, me).wait_send()
    for d in range(1, groups):
        modes_copy(lax.rem(grp + d, groups), grp).wait_send()


def pieces(x):
    hi = x.astype(jnp.bfloat16)
    rest = x - hi.astype(jnp.float32)
    mid = rest.astype(jnp.bfloat16)
    return hi, mid, (rest - mid.astype(jnp.float32)).astype(jnp.bfloat16)


def residual_kernel(vis_ref, modes_ref, coef_ref, out_ref):
    width = coef_ref.shape[2]
    hi, mid, lo = pieces(modes_ref[...])
    left = jnp.concatenate([hi, hi, mid, mid, hi, lo], axis=0)
    for j in range(coef_ref.shape[0]):
        cols = slice(j * width, (j + 1) * width)
        hi, mid, lo = pieces(coef_ref[j])
        right = jnp.concatenate([hi, mid, hi, mid, lo, hi], axis=0)
        out_ref[:, cols] = vis_ref[:, cols] - lax.dot_general(
            left, right, (((0,), (0,)), ((), ())), preferred_element_type=jnp.float32)


def per_device(chan, groups, visibility, interference_mask, valid_time_count, fit_modes):
    rows, all_columns = visibility.shape
    freqs, columns = interference_mask.shape
    share, modes = fit_modes.shape
    base = valid_time_count.shape[0]
    times = columns // base
    width = 2 * columns
    chips = chan // 2
    within = (lax.broadcasted_iota(jnp.int32, (base, times), 1) < valid_time_count[:, None]).astype(jnp.float32)
    valid = within.reshape(1, columns)
    valid_wide = jnp.broadcast_to(within[:, None, :], (base, 2, times)).reshape(1, width)
    source = lax.broadcasted_iota(jnp.int32, (LANES, 2 * LANES), 0)
    column = lax.broadcasted_iota(jnp.int32, (LANES, 2 * LANES), 1)
    spread = (source == column // (2 * times) * times + column % times).astype(jnp.bfloat16)
    f32, bf16 = jnp.float32, jnp.bfloat16
    block = pltpu.VMEM((chips, modes, width), f32)
    anywhere = pl.BlockSpec(memory_space=pl.ANY)
    coefficients, local = pl.pallas_call(
        functools.partial(fit_kernel, chips, groups),
        out_shape=(jax.ShapeDtypeStruct((chan, modes, width), f32), jax.ShapeDtypeStruct((modes, rows), f32)),
        in_specs=[anywhere] * 2 + [VMEM] * 4,
        out_specs=(VMEM, VMEM),
        scratch_shapes=[
            pltpu.VMEM((rows, all_columns), f32),
            pltpu.VMEM((freqs, columns), jnp.int32),
            pltpu.VMEM((chan, rows, columns), jnp.int32),
            pltpu.VMEM((groups, modes, share), f32),
            pltpu.VMEM((modes, freqs), f32),
            pltpu.VMEM((freqs, width), bf16),
        ]
        + [pltpu.VMEM((modes * modes, freqs), bf16)] * 3
        + [pltpu.VMEM((modes, modes, width), f32), pltpu.VMEM((modes, width), f32)]
        + [block] * 5
        + [pltpu.SemaphoreType.DMA((8, chips)), pltpu.SemaphoreType.DMA((2, chan)),
           pltpu.SemaphoreType.DMA((2, groups)), pltpu.SemaphoreType.DMA((3,))],
        compiler_params=pltpu.CompilerParams(
            collective_id=0, has_side_effects=True, vmem_limit_bytes=61 << 20),
        cost_estimate=pl.CostEstimate(flops=10**10, bytes_accessed=12 << 20, transcendentals=0),
        name="fit",
    )(visibility, interference_mask, fit_modes.T, spread, valid, valid_wide)
    step = 2
    return pl.pallas_call(
        residual_kernel,
        grid=(chan // step,),
        out_shape=jax.ShapeDtypeStruct((rows, all_columns), f32),
        in_specs=[
            pl.BlockSpec((rows, step * width), lambda i: (0, i)),
            pl.BlockSpec((modes, rows), lambda i: (0, 0)),
            pl.BlockSpec((step, modes, width), lambda i: (i, 0, 0)),
        ],
        out_specs=pl.BlockSpec((rows, step * width), lambda i: (0, i)),
        name="residual",
    )(visibility, local, coefficients)


def solution(mesh):
    placed = (P("chan", "grp"), P(None, ("grp", "chan")), P(("grp", "chan")), P("grp", None))
    return jax.shard_map(
        functools.partial(per_device, mesh.shape["chan"], mesh.shape["grp"]), mesh=mesh, in_specs=placed,
        out_specs=P("chan", "grp"), check_vma=False)
```
